128 devices in a mesh: group: 4 (over y), leaf: 32 (over x, z, core).
Axes of the slice: x: 4, y: 4, z: 4, core: 2. Of those that a mesh axis runs over, the one named last changes fastest.
Arguments:
- points: bfloat16 [262144, 64], P(('group', 'leaf')), may hold values from -1.1953125 to 1.1953125
- ordering: int32 [128, 2048], P(('group', 'leaf')), may hold values from 0 to 2047, each once within a row
- iterate: float32 [262144, 128], P(('group', 'leaf')), may hold values from -6 to 6
- target: float32 [262144, 128], P(('group', 'leaf')), may hold values from -18 to 18
- step_size: float32 [128], replicated, may hold values from 0.1 to 0.5
- leaf_basis: bfloat16 [262144, 256], P(('group', 'leaf')), may hold values from -0.125 to 0.125
- transfer: bfloat16 [128, 256, 256], P(('group', 'leaf')), may hold values from -0.375 to 0.375
- leaf_skeleton: bfloat16 [128, 256, 64], P(('group', 'leaf')), may hold values from -0.8984375 to 0.8984375
- cluster_skeleton: bfloat16 [4, 256, 64], P('group'), may hold values from -1.1953125 to 1.1953125
- near_table: int32 [128, 32], P(('group', 'leaf')), may hold values from 0 to 1, as said below
- far_table: int32 [128, 32], P(('group', 'leaf')), may hold values from 0 to 1, as said below
- cluster_far: int32 [4, 4], P('group'), may hold values from 0 to 1, as said below
Outputs:
- updated: float32 [262144, 128], P(('group', 'leaf'))
The draws below stay inside these ranges and needn't reach their ends.
Inputs may be any that keep to these rules, and one draw needn't show every extreme that they name: `near_table`: entries 0 or 1; each leaf's own place is 1; a 1 stands only at places at most 3 away from the leaf's own place; each row has at most 7 ones, and some row exactly 7. `far_table`: entries 0 or 1, never 1 where near_table is 1. `cluster_far`: entries 0 or 1, zero on the diagonal. `ordering`: each row is a permutation.
All inputs are finite; a program needn't handle non-finite values.
Results may differ from the reference program's by a relative error of at most 0.0044.
Values may be sent and summed in bfloat16 or wider, within the bound.
A program may use at most 128 MiB of HBM per device.

```python
import math
import jax
import jax.numpy as jnp
from jax import lax

DIM = 64
RANK = 256
NRHS = 128
LEAF = 2048
NEAR_MOST = 7
CLUSTER = 32
GROUPS = 4
LEAVES = 128
POINTS = 262144


def near_pattern(key):
    reach = (NEAR_MOST - 1) // 2
    leaf_ids = jnp.arange(LEAVES, dtype=jnp.int32)
    own_place = leaf_ids % CLUSTER
    places = jnp.arange(CLUSTER, dtype=jnp.int32)
    base_key = jax.random.fold_in(key, 11)
    coin_key, group_key, place_key = jax.random.split(base_key, 3)
    distance = jnp.abs(places[None, :] - own_place[:, None])
    within = (distance <= reach) & (distance > 0)
    coins = jax.random.randint(coin_key, (LEAVES, CLUSTER), 0, 2)
    busy_group = jax.random.randint(group_key, (), 0, GROUPS)
    busy_place = jax.random.randint(place_key, (), reach, CLUSTER - reach)
    busiest = busy_group * CLUSTER + busy_place
    coins = jnp.where((leaf_ids == busiest)[:, None], 1, coins)
    chosen = (distance == 0) | within & (coins > 0)
    return chosen.astype(jnp.int32)


def draw_near_table(key, part):
    return near_pattern(key)


def draw_far_table(key, part):
    nearby = near_pattern(key)
    dice_roll = jax.random.randint(jax.random.fold_in(key, 12), (LEAVES, CLUSTER), 0, 4)
    return ((nearby == 0) & (dice_roll > 0)).astype(jnp.int32)


def draw_cluster_far(key, part):
    dice_roll = jax.random.randint(jax.random.fold_in(key, 13), (GROUPS, GROUPS), 0, 3)
    ids = jnp.arange(GROUPS, dtype=jnp.int32)
    return ((dice_roll > 0) & (ids[:, None] != ids[None, :])).astype(jnp.int32)


def level_of(own_key, dims, shards, low, high):
    factor_of = 1.0
    for dim, shards_of in shards:
        heights = jax.random.uniform(jax.random.fold_in(jax.random.fold_in(own_key, 6), dim), (shards_of,), jnp.float32, low / len(shards), high / len(shards))
        factor_of = factor_of * jnp.repeat(jnp.exp(heights), dims[dim] // shards_of).reshape((-1,) + (1,) * (len(dims) - 1 - dim))
    return factor_of


def scatter_about(stream_key, dims, width, most, cuts=(), held_as=jnp.bfloat16):
    entries = width * jax.random.normal(stream_key, dims, jnp.float32)
    if cuts:
        entries = entries * level_of(stream_key, dims, cuts, -0.22, 0.18)
    return jnp.clip(entries, -most, most).astype(held_as)


def setup_inputs(seed: int = 0) -> dict:
    key_of = jax.random.split(jax.random.key(seed), 13)
    return {
        "points": scatter_about(key_of[0], (POINTS, DIM), 0.2, 1.1953125, ((0, 128),)),
        "ordering": jax.vmap(lambda own: jax.random.permutation(own, LEAF))(jax.random.split(key_of[1], LEAVES)).reshape((LEAVES, LEAF)).astype(jnp.int32),
        "iterate": scatter_about(key_of[2], (POINTS, NRHS), 1.0, 6.0, ((0, 128),), jnp.float32),
        "target": scatter_about(key_of[3], (POINTS, NRHS), 3.0, 18.0, ((0, 128),), jnp.float32),
        "step_size": jnp.clip(jnp.exp(jax.random.uniform(key_of[4], (NRHS,), jnp.float32, math.log(0.1), math.log(0.5))), 0.1, 0.5),
        "leaf_basis": scatter_about(key_of[5], (POINTS, RANK), LEAF ** -0.5, 0.125, ((0, 128),)),
        "transfer": scatter_about(key_of[6], (LEAVES, RANK, RANK), RANK ** -0.5, 0.375, ((0, 128),)),
        "leaf_skeleton": scatter_about(key_of[7], (LEAVES, RANK, DIM), 0.15, 0.8984375, ((0, 128),)),
        "cluster_skeleton": scatter_about(key_of[8], (GROUPS, RANK, DIM), 0.2, 1.1953125, ((0, 4),)),
        "near_table": draw_near_table(jax.random.fold_in(key_of[12], 71), 0),
        "far_table": draw_far_table(jax.random.fold_in(key_of[12], 71), 0),
        "cluster_far": draw_cluster_far(jax.random.fold_in(key_of[12], 71), 0),
    }


def kernel_tile(left, right):
    left_f = left.astype(jnp.float32)
    right_f = right.astype(jnp.float32)
    left_sq = jnp.sum(left_f * left_f, axis=1)
    right_sq = jnp.sum(right_f * right_f, axis=1)
    inner = lax.dot_general(left, right, (((1,), (1,)), ((), ())), preferred_element_type=jnp.float32)
    return jnp.exp(-(left_sq[:, None] + right_sq[None, :] - 2.0 * inner)).astype(jnp.bfloat16)


def reference(points, ordering, iterate, target, step_size, leaf_basis, transfer, leaf_skeleton, cluster_skeleton, near_table, far_table, cluster_far):
    cloud = points.reshape(LEAVES, LEAF, DIM)
    rounded = iterate.astype(jnp.bfloat16).reshape(LEAVES, LEAF, NRHS)
    basis = leaf_basis.reshape(LEAVES, LEAF, RANK)
    coeffs = lax.map(lambda operands: jnp.dot(operands[0].T, operands[1], preferred_element_type=jnp.float32), (basis, rounded)).astype(jnp.bfloat16)

    def near_leaf(leaf_id):
        first_leaf = (leaf_id // CLUSTER) * CLUSTER
        own_points = cloud[leaf_id]

        def visit(place, running):
            other = first_leaf + place

            def include(summed):
                return summed + jnp.dot(kernel_tile(own_points, cloud[other]), rounded[other], preferred_element_type=jnp.float32)
            return lax.cond(near_table[leaf_id, place] > 0, include, lambda summed: summed, running)
        return lax.fori_loop(0, CLUSTER, visit, jnp.zeros((LEAF, NRHS), jnp.float32))

    def far_leaf(leaf_id):
        first_leaf = (leaf_id // CLUSTER) * CLUSTER
        own_skeleton = leaf_skeleton[leaf_id]

        def visit(place, running):
            other = first_leaf + place

            def include(summed):
                return summed + jnp.dot(kernel_tile(own_skeleton, leaf_skeleton[other]), coeffs[other], preferred_element_type=jnp.float32)
            return lax.cond(far_table[leaf_id, place] > 0, include, lambda summed: summed, running)
        return lax.fori_loop(0, CLUSTER, visit, jnp.zeros((RANK, NRHS), jnp.float32))

    leaf_ids = jnp.arange(LEAVES, dtype=jnp.int32)
    near_sum = lax.map(near_leaf, leaf_ids)
    far_sum = lax.map(far_leaf, leaf_ids)
    upward_terms = lax.map(lambda operands: jnp.dot(operands[0].T, operands[1], preferred_element_type=jnp.float32), (transfer, coeffs))
    upper = jnp.sum(upward_terms.reshape(GROUPS, CLUSTER, RANK, NRHS), axis=1).astype(jnp.bfloat16)

    def cluster_row(group_id):
        def visit(other, running):
            def include(summed):
                return summed + jnp.dot(kernel_tile(cluster_skeleton[group_id], cluster_skeleton[other]), upper[other], preferred_element_type=jnp.float32)
            return lax.cond(cluster_far[group_id, other] > 0, include, lambda summed: summed, running)
        return lax.fori_loop(0, GROUPS, visit, jnp.zeros((RANK, NRHS), jnp.float32))

    lower = lax.map(cluster_row, jnp.arange(GROUPS, dtype=jnp.int32)).astype(jnp.bfloat16)
    parent = jnp.repeat(lower, CLUSTER, axis=0)
    local = (far_sum + lax.map(lambda operands: jnp.dot(operands[0], operands[1], preferred_element_type=jnp.float32), (transfer, parent))).astype(jnp.bfloat16)
    image = lax.map(lambda operands: jnp.dot(operands[0], operands[1], preferred_element_type=jnp.float32), (basis, local)) + near_sum
    sorted_target = jnp.take_along_axis(target.reshape(LEAVES, LEAF, NRHS), ordering[:, :, None].astype(jnp.int32), axis=1)
    updated = iterate.reshape(LEAVES, LEAF, NRHS) + step_size[None, None, :] * (sorted_target - image)
    return updated.reshape(POINTS, NRHS)
```

```python
import jax
import jax.numpy as jnp
from jax import lax
from jax.experimental import pallas as pl
from jax.experimental.pallas import tpu as pltpu
from jax.sharding import PartitionSpec as P

LEAF, DIM, NRHS, RANK, CLUSTER, GROUPS = 2048, 64, 128, 256, 32, 4
HALF_LEAF = LEAF // 2
LANES = 128
CHUNKS = 4
QH = HALF_LEAF // CHUNKS
CHUNK_ROWS = 3 * QH
BLOCKS = QH // LANES
LOG2E = 1.4426950408889634
BIG = 1.0e4
POINT_SHIFT, LEAF_SHIFT, CLUSTER_SHIFT = 45.0, 25.0, 45.0
OWN, PARTNER, DOWN, UP, PARTNER_DOWN, PARTNER_UP, FAR_SIDE = range(7)
F32, BF16 = jnp.float32, jnp.bfloat16


def dot(a, b):
    return jnp.dot(a, b, preferred_element_type=F32)


def packed(rows):
    half = rows.shape[0] // 2
    return jnp.concatenate([rows[:half], rows[half:]], axis=1)


def stationary(pack_t, shift):
    doubled = pack_t + pack_t
    zeros = jnp.zeros_like(doubled[:DIM])
    low, high = doubled[:DIM], doubled[DIM:]
    both = jnp.concatenate([low, high], axis=1)
    empty = jnp.concatenate([zeros, zeros], axis=1)
    first = jnp.concatenate([both, empty], axis=0).astype(BF16)
    second = jnp.concatenate([empty, both], axis=0).astype(BF16)
    squares = pack_t * pack_t
    norm = jnp.concatenate(
        [jnp.sum(squares[:DIM], axis=0, keepdims=True), jnp.sum(squares[DIM:], axis=0, keepdims=True)],
        axis=1,
    )
    return first, second, (norm + shift) * LOG2E, jnp.exp2((shift - norm) * LOG2E)


def kernel(
    points, ordering, iterate, target, step, basis, transfer, leaf_skel, cluster_skel,
    near_table, far_table, cluster_far,
    out,
    nb, at, exponent, values, near, gathered, skel_at, skel_exp, far_acc,
    up_own, up_pair, up_z, up_x, yb, cluster_at, cluster_exp, low,
    near_send, near_recv, gat_send, gat_recv, up_send, up_recv, y_send, y_recv,
):
    g = lax.axis_index("group")
    l = lax.axis_index("leaf")
    x, z, k = l // 8, (l // 2) % 4, l % 2

    def at_leaf(xx, zz):
        return (xx % 4) * 8 + (zz % 4) * 2 + k

    partner = x * 8 + z * 2 + (1 - k)
    above, below = (l + 2) % CLUSTER, (l + CLUSTER - 2) % CLUSTER
    side = (l + CLUSTER + 2 * k - 1) % CLUSTER
    z_peers = [at_leaf(x, z + 1), at_leaf(x, z + 3), at_leaf(x, z + 2)]
    x_peers = [at_leaf(x + 1, z), at_leaf(x + 3, z), at_leaf(x + 2, z)]
    y_peers = [(g + 1) % GROUPS, (g + 3) % GROUPS, (g + 2) % GROUPS]

    barrier = pltpu.get_barrier_semaphore()
    for leaf in [partner, above, below, side] + z_peers + x_peers:
        pl.semaphore_signal(barrier, 1, device_id={"leaf": leaf}, device_id_type=pl.DeviceIdType.MESH)
    for group in y_peers:
        pl.semaphore_signal(barrier, 1, device_id={"group": group}, device_id_type=pl.DeviceIdType.MESH)

    def remote(src, dst, send, recv, leaf=None, group=None):
        return pltpu.make_async_remote_copy(
            src_ref=src, dst_ref=dst, send_sem=send, recv_sem=recv,
            device_id={"leaf": leaf} if group is None else {"group": group},
            device_id_type=pl.DeviceIdType.MESH,
        )

    for c in range(CHUNKS):
        rows = slice(c * QH, (c + 1) * QH)
        rows_high = slice(HALF_LEAF + c * QH, HALF_LEAF + (c + 1) * QH)
        nb[OWN, c, 0:QH, :] = jnp.concatenate([points[rows, :], points[rows_high, :]], axis=1)
    pack_t = jnp.concatenate(
        [nb[OWN, c, 0:QH, :].astype(F32).T for c in range(CHUNKS)], axis=1
    )
    first, second, exponent_row, scale = stationary(pack_t, POINT_SHIFT)
    at[0] = first
    at[1] = second
    exponent[...] = exponent_row
    for i in range(LEAF // LANES):
        block = iterate[i * LANES:(i + 1) * LANES, :].astype(BF16).astype(F32).T
        values[:, i * LANES:(i + 1) * LANES] = block.astype(BF16)
        high, j = divmod(i, HALF_LEAF // LANES)
        c, b = divmod(j, BLOCKS)
        start = QH + LANES * (high * BLOCKS + b)
        nb[OWN, c, start:start + LANES, :] = (
            block * scale[:, i * LANES:(i + 1) * LANES]
        ).astype(BF16)

    pl.semaphore_wait(barrier, 13)

    def near_copy(kind, c):
        src, dst, leaf = [
            (OWN, PARTNER, partner),
            (OWN, DOWN, above),
            (OWN, UP, below),
            (DOWN, PARTNER_DOWN, partner),
            (UP, PARTNER_UP, partner),
            (DOWN + 1 - k, FAR_SIDE, side),
        ][kind]
        return remote(nb.at[src, c], nb.at[dst, c], near_send.at[kind, c], near_recv.at[dst - 1, c], leaf)

    def send_near(kinds, c):
        for kind in kinds:
            near_copy(kind, c).start()

    def near_arrived(kinds, c):
        for kind in kinds:
            near_copy(kind, c).wait_recv()

    for c in range(CHUNKS):
        send_near([0], c)
    send_near([1, 2], 0)

    coef = dot(values[...], basis[...]).astype(BF16)
    skel_pack = packed(leaf_skel[0])
    first, second, exponent_row, scale = stationary(skel_pack.astype(F32).T, LEAF_SHIFT)
    skel_at[0] = first
    skel_at[1] = second
    skel_exp[...] = exponent_row
    scaled = (coef.astype(F32) * scale).astype(BF16)
    gathered[k, x, z, 0:LANES, :] = skel_pack
    gathered[k, x, z, LANES:2 * LANES, :] = scaled[:, :LANES]
    gathered[k, x, z, 2 * LANES:, :] = scaled[:, LANES:]
    z_from = [(z + 3) % 4, (z + 1) % 4, (z + 2) % 4]

    def gather_z(i):
        own = gathered.at[k, x, z]
        return remote(own, own, gat_send.at[i], gat_recv.at[i], z_peers[i])

    for i in range(3):
        gather_z(i).start()
    lifted = dot(coef, transfer[0])
    up_own[0] = lifted[:NRHS // 2]
    up_own[1] = lifted[NRHS // 2:]
    pair_copy = remote(up_own.at[1 - k], up_pair, up_send.at[0], up_recv.at[0], partner)
    pair_copy.start()
    send_near([1, 2], 1)

    near[...] = jnp.zeros_like(near)

    def near_chunk(slot, c, place):
        inside = (place >= 0) & (place < CLUSTER)
        listed = near_table[0, (place + CLUSTER) % CLUSTER] * inside.astype(jnp.int32)
        row = exponent[...] + (1.0 - listed.astype(F32)) * BIG
        points_c = nb[slot, c, 0:QH, :]

        def weights(h):
            s = dot(points_c, at[h])
            return jnp.exp2(s * LOG2E - row).astype(BF16)

        def value(h):
            start = QH + h * BLOCKS * LANES
            return jnp.concatenate(
                [nb[slot, c, start + b * LANES:start + (b + 1) * LANES, :] for b in range(BLOCKS)], axis=1
            )

        low_w = weights(0)
        high_w = weights(1)
        near[...] += dot(value(0), low_w)
        near[...] += dot(value(1), high_w)

    def whole(slot, place):
        def visit(c, carry):
            near_chunk(slot, c, place)
            return carry

        lax.fori_loop(0, CHUNKS, visit, 0)

    def stage(c):
        near_arrived([3, 4], c)

        def visit(slot, carry):
            other = jnp.where(slot >= PARTNER_DOWN, l + 1 - 2 * k, l)
            place = other + 4 * (slot % 2) - 2
            near_chunk(slot, c, place)
            return carry

        lax.fori_loop(DOWN, PARTNER_UP + 1, visit, 0)

    def forward(c):
        near_arrived([1, 2], c)
        send_near([3, 4, 5], c)

    whole(OWN, l)

    pair_copy.wait_recv()
    up_z[0] = up_own[k] + up_pair[...]

    def up_copy_z(i):
        return remote(up_z.at[0], up_z.at[i + 1], up_send.at[1 + i], up_recv.at[1 + i], z_peers[i])

    def up_copy_x(i):
        return remote(up_x.at[0], up_x.at[i + 1], up_send.at[4 + i], up_recv.at[4 + i], x_peers[i])

    for i in range(3):
        up_copy_z(i).start()

    def gather_x(i):
        own = gathered.at[k, x]
        return remote(own, own, gat_send.at[3 + i], gat_recv.at[3 + i], x_peers[i])

    def gather_relay(i):
        column = (x + 3) % 4 if i == 0 else (x + 1) % 4
        part = gathered.at[k, column, pl.ds(2 * i, 2)]
        return remote(part, part, gat_send.at[5 + i], gat_recv.at[5 + i], x_peers[i])

    def gather_pair(i):
        column = (x + i) % 4
        part = gathered.at[k, column]
        return remote(part, part, gat_send.at[7 + i], gat_recv.at[7 + i], partner)

    for i in range(3):
        gather_z(i).wait_recv()
    for i in range(2):
        gather_x(i).start()
    gather_pair(0).start()
    send_near([1, 2], 2)
    forward(0)
    near_arrived([0], 0)
    near_arrived([0], 1)
    near_arrived([0], 2)
    near_arrived([0], 3)
    whole(PARTNER, l + 1 - 2 * k)

    send_near([1, 2], 3)
    forward(1)
    for i in range(3):
        up_copy_z(i).wait_recv()
    up_x[0] = (up_z[0] + up_z[1]) + (up_z[2] + up_z[3])
    for i in range(3):
        up_copy_x(i).start()
    stage(0)

    forward(2)
    for i in range(2):
        gather_x(i).wait_recv()
    for i in range(2):
        gather_relay(i).start()
    gather_pair(1).start()
    gather_pair(3).start()
    for i in range(3):
        up_copy_x(i).wait_recv()
    upper = ((up_x[0] + up_x[1]) + (up_x[2] + up_x[3])).astype(BF16)
    cluster_pack = packed(cluster_skel[0])
    first, second, exponent_row, scale = stationary(cluster_pack.astype(F32).T, CLUSTER_SHIFT)
    cluster_at[0] = first
    cluster_at[1] = second
    cluster_exp[...] = exponent_row
    scaled = (upper.astype(F32) * scale).astype(BF16)
    yb[g, 0:LANES, :] = cluster_pack
    yb[g, LANES:LANES + NRHS // 2, :] = scaled[:, :LANES]
    yb[g, LANES + NRHS // 2:, :] = scaled[:, LANES:]

    def y_copy(i):
        return remote(yb.at[g], yb.at[g], y_send.at[i], y_recv.at[i], group=y_peers[i])

    for i in range(3):
        y_copy(i).start()
    stage(1)

    forward(3)
    for i in range(3):
        y_copy(i).wait_recv()

    def block_weights(pack, stationary_ref, row):
        return jnp.concatenate(
            [jnp.exp2(dot(pack, stationary_ref[h]) * LOG2E - row).astype(BF16) for h in range(2)], axis=0
        )

    lower = jnp.zeros((NRHS // 2, RANK), F32)
    for h in range(GROUPS):
        row = cluster_exp[...] + (1.0 - cluster_far[0, h].astype(F32)) * BIG
        weights = block_weights(yb[h, 0:LANES, :], cluster_at, row)
        value = jnp.concatenate(
            [yb[h, LANES:LANES + NRHS // 2, :], yb[h, LANES + NRHS // 2:, :]], axis=1
        )
        lower = lower + dot(value, weights)
    low[k] = lower.astype(BF16)
    low_copy = remote(low.at[k], low.at[k], y_send.at[3], y_recv.at[3], partner)
    low_copy.start()
    stage(2)

    for i in range(2):
        gather_relay(i).wait_recv()
    gather_pair(2).start()
    stage(3)

    for i in range(4):
        gather_pair(i).wait_recv()
    far_acc[...] = jnp.zeros_like(far_acc)

    def far_visit(n, carry):
        kk, xx = n // 4, n % 4
        total = jnp.zeros((NRHS, RANK), F32)
        for zz in range(4):
            row = skel_exp[...] + (1.0 - far_table[0, xx * 8 + zz * 2 + kk].astype(F32)) * BIG
            weights = block_weights(gathered[kk, xx, zz, 0:LANES, :], skel_at, row)
            value = jnp.concatenate(
                [gathered[kk, xx, zz, LANES:2 * LANES, :], gathered[kk, xx, zz, 2 * LANES:, :]], axis=1
            )
            total = total + dot(value, weights)
        far_acc[...] += total
        return carry

    lax.fori_loop(0, 8, far_visit, 0)
    low_copy.wait_recv()
    lower_all = jnp.concatenate([low[0], low[1]], axis=0)
    local_t = far_acc[...] + lax.dot_general(
        lower_all, transfer[0], (((1,), (1,)), ((), ())), preferred_element_type=F32
    )
    local = local_t.astype(BF16).astype(F32).T.astype(BF16)

    def pick(i, carry):
        for j in range(8):
            out[pl.ds(i * 8 + j, 1), :] = target[pl.ds(ordering[0, i * 8 + j], 1), :]
        return carry

    lax.fori_loop(0, LEAF // 8, pick, 0)

    def last(c, carry):
        near_copy(5, c).wait_recv()
        near_chunk(FAR_SIDE, c, l + 6 * k - 3)
        return carry

    lax.fori_loop(0, CHUNKS, last, 0)
    for i in range(LEAF // LANES):
        rows = slice(i * LANES, (i + 1) * LANES)
        image = dot(basis[rows, :], local) + near[:, rows].T
        out[rows, :] = iterate[rows, :] + step[...] * (out[rows, :] - image)

    for kind in range(6):
        for c in range(CHUNKS):
            near_copy(kind, c).wait_send()
    for i in range(3):
        gather_z(i).wait_send()
        up_copy_z(i).wait_send()
        up_copy_x(i).wait_send()
        y_copy(i).wait_send()
    for i in range(2):
        gather_x(i).wait_send()
        gather_relay(i).wait_send()
    for i in range(4):
        gather_pair(i).wait_send()
    pair_copy.wait_send()
    low_copy.wait_send()


def body(
    points, ordering, iterate, target, step_size, leaf_basis, transfer, leaf_skeleton,
    cluster_skeleton, near_table, far_table, cluster_far,
):
    vmem = pl.BlockSpec(memory_space=pltpu.VMEM)
    smem = pl.BlockSpec(memory_space=pltpu.SMEM)
    dma = pltpu.SemaphoreType.DMA
    return pl.pallas_call(
        kernel,
        out_shape=jax.ShapeDtypeStruct((LEAF, NRHS), F32),
        in_specs=[vmem, smem, vmem, vmem, vmem, vmem, vmem, vmem, vmem, smem, smem, smem],
        out_specs=vmem,
        scratch_shapes=[
            pltpu.VMEM((7, CHUNKS, CHUNK_ROWS, LANES), BF16),
            pltpu.VMEM((2, LANES, LEAF), BF16),
            pltpu.VMEM((1, LEAF), F32),
            pltpu.VMEM((NRHS, LEAF), BF16),
            pltpu.VMEM((NRHS, LEAF), F32),
            pltpu.VMEM((2, 4, 4, 3 * LANES, LANES), BF16),
            pltpu.VMEM((2, LANES, RANK), BF16),
            pltpu.VMEM((1, RANK), F32),
            pltpu.VMEM((NRHS, RANK), F32),
            pltpu.VMEM((2, NRHS // 2, RANK), F32),
            pltpu.VMEM((NRHS // 2, RANK), F32),
            pltpu.VMEM((4, NRHS // 2, RANK), F32),
            pltpu.VMEM((4, NRHS // 2, RANK), F32),
            pltpu.VMEM((GROUPS, LANES + NRHS, LANES), BF16),
            pltpu.VMEM((2, LANES, RANK), BF16),
            pltpu.VMEM((1, RANK), F32),
            pltpu.VMEM((2, NRHS // 2, RANK), BF16),
            dma((6, CHUNKS)), dma((6, CHUNKS)),
            dma((11,)), dma((11,)),
            dma((7,)), dma((7,)),
            dma((4,)), dma((4,)),
        ],
        compiler_params=pltpu.CompilerParams(
            collective_id=0, has_side_effects=True, vmem_limit_bytes=56 * 2**20
        ),
    )(
        points, ordering, iterate, target, step_size[None, :], leaf_basis, transfer,
        leaf_skeleton, cluster_skeleton, near_table, far_table, cluster_far,
    )


def solution(mesh):
    both = ("group", "leaf")
    return jax.shard_map(
        body,
        mesh=mesh,
        in_specs=(
            P(both, None), P(both, None), P(both, None), P(both, None), P(), P(both, None),
            P(both, None, None), P(both, None, None), P("group", None, None),
            P(both, None), P(both, None), P("group", None),
        ),
        out_specs=P(both, None),
        check_vma=False,
    )
```

```python
import jax
import jax.numpy as jnp
from jax import lax
from jax.experimental import pallas as pl
from jax.experimental.pallas import tpu as pltpu
from jax.sharding import PartitionSpec as P

LEAF, DIM, NRHS, RANK, CLUSTER, GROUPS = 2048, 64, 128, 256, 32, 4
HALF_LEAF = LEAF // 2
LANES = 128
CHUNKS = 4
QH = HALF_LEAF // CHUNKS
CHUNK_ROWS = 3 * QH
BLOCKS = QH // LANES
LOG2E = 1.4426950408889634
BIG = 1.0e4
POINT_SHIFT, LEAF_SHIFT, CLUSTER_SHIFT = 45.0, 25.0, 45.0
OWN, PARTNER, DOWN, UP, PARTNER_DOWN, PARTNER_UP, FAR_SIDE = range(7)
F32, BF16 = jnp.float32, jnp.bfloat16


def dot(a, b):
    return jnp.dot(a, b, preferred_element_type=F32)


def stacked(cols):
    half = cols.shape[1] // 2
    return jnp.concatenate([cols[:, :half], cols[:, half:]], axis=0)


def exponent_and_scale(cols, shift):
    norm = jnp.sum(cols * cols, axis=0, keepdims=True)
    return (norm + shift) * LOG2E, jnp.exp2((shift - norm) * LOG2E)


def fill_stationary(ref, doubled):
    zeros = jnp.zeros_like(doubled)
    ref[0, 0:DIM, :] = doubled
    ref[0, DIM:, :] = zeros
    ref[1, 0:DIM, :] = zeros
    ref[1, DIM:, :] = doubled


def kernel(
    points, ordering, iterate, target, step, basis, transfer, leaf_skel, cluster_skel,
    near_table, far_table, cluster_far,
    out,
    nb, at, exponent, values, near, gathered, row_skel, row_exp, own_exp, row_at, far_total, far_out, far_in,
    up_total, up_out, up_in, yb, cluster_at, cluster_exp, low,
    near_send, near_recv, gat_send, gat_recv, row_send, row_recv, up_send, up_recv, y_send, y_recv,
):
    g = lax.axis_index("group")
    l = lax.axis_index("leaf")
    x, z, k = l // 8, (l // 2) % 4, l % 2
    half = NRHS // 2

    def at_leaf(xx, zz):
        return (xx % 4) * 8 + (zz % 4) * 2 + k

    partner = x * 8 + z * 2 + (1 - k)
    above, below = (l + 2) % CLUSTER, (l + CLUSTER - 2) % CLUSTER
    side = (l + CLUSTER + 2 * k - 1) % CLUSTER
    z_even, x_even = z % 2, x % 2
    z_first, z_second = at_leaf(x, z + 1 - 2 * z_even), at_leaf(x, z + 3 + 2 * z_even)
    x_first, x_second = at_leaf(x + 1 - 2 * x_even, z), at_leaf(x + 3 + 2 * x_even, z)
    x_peers = [at_leaf(x + i, z) for i in range(1, 4)]
    y_peers = [(g + i) % GROUPS for i in range(1, 4)]

    barrier = pltpu.get_barrier_semaphore()
    for leaf in [partner, above, below, side, z_first, z_second] + x_peers:
        pl.semaphore_signal(barrier, 1, device_id={"leaf": leaf}, device_id_type=pl.DeviceIdType.MESH)
    for group in y_peers:
        pl.semaphore_signal(barrier, 1, device_id={"group": group}, device_id_type=pl.DeviceIdType.MESH)

    def remote(src, dst, send, recv, leaf=None, group=None):
        return pltpu.make_async_remote_copy(
            src_ref=src, dst_ref=dst, send_sem=send, recv_sem=recv,
            device_id={"leaf": leaf} if group is None else {"group": group},
            device_id_type=pl.DeviceIdType.MESH,
        )

    cols = points[...].astype(F32)
    stack = stacked(cols)
    for c in range(CHUNKS):
        nb[OWN, c, 0:QH, :] = stack[:, c * QH:(c + 1) * QH].T.astype(BF16)
    fill_stationary(at, (cols + cols).astype(BF16))
    exponent_row, scale = exponent_and_scale(cols, POINT_SHIFT)
    exponent[...] = exponent_row
    for i in range(LEAF // LANES):
        block = iterate[i * LANES:(i + 1) * LANES, :].astype(BF16).astype(F32).T
        values[:, i * LANES:(i + 1) * LANES] = block.astype(BF16)
        high, j = divmod(i, HALF_LEAF // LANES)
        c, b = divmod(j, BLOCKS)
        start = QH + LANES * (high * BLOCKS + b)
        nb[OWN, c, start:start + LANES, :] = (
            block * scale[:, i * LANES:(i + 1) * LANES]
        ).astype(BF16)

    pl.semaphore_wait(barrier, 12)

    def near_copy(kind, c):
        src, dst, leaf = [
            (OWN, PARTNER, partner),
            (OWN, DOWN, above),
            (OWN, UP, below),
            (DOWN, PARTNER_DOWN, partner),
            (UP, PARTNER_UP, partner),
            (DOWN + 1 - k, FAR_SIDE, side),
        ][kind]
        return remote(nb.at[src, c], nb.at[dst, c], near_send.at[kind, c], near_recv.at[dst - 1, c], leaf)

    def send_near(kinds, c):
        for kind in kinds:
            near_copy(kind, c).start()

    def near_arrived(kinds, c):
        for kind in kinds:
            near_copy(kind, c).wait_recv()

    send_near([1, 2], 0)
    for c in range(CHUNKS):
        send_near([0], c)

    coef = dot(values[...], basis[...]).astype(BF16)
    skel = leaf_skel[0].astype(F32)
    skel_row, scale = exponent_and_scale(skel, LEAF_SHIFT)
    scaled = (coef.astype(F32) * scale).astype(BF16)
    gathered[k, z, 0:LANES, :] = stacked(skel).T.astype(BF16)
    gathered[k, z, LANES:2 * LANES, :] = scaled[:, :LANES]
    gathered[k, z, 2 * LANES:, :] = scaled[:, LANES:]

    def gather_copy(i):
        part = [gathered.at[k, z], gathered.at[k, pl.ds(2 * (z // 2), 2)], gathered.at[k]][i]
        return remote(part, part, gat_send.at[i], gat_recv.at[i], [z_first, z_second, partner][i])

    gather_copy(0).start()
    lifted = dot(coef, transfer[0])
    for i in range(2):
        up_total[i] = lifted[i * half:(i + 1) * half]
        up_out[i] = lifted[i * half:(i + 1) * half].astype(BF16)

    def up_copy(i):
        src = up_out.at[1 - k] if i == 0 else up_out.at[i + 1]
        leaf = [partner, z_first, z_second, x_first, x_second][i]
        return remote(src, up_in.at[i], up_send.at[i], up_recv.at[i], leaf)

    up_copy(0).start()

    row_skel[x] = (skel + skel).astype(BF16)
    for xx in range(4):
        for j in range(8):
            own_exp[xx, j:j + 1, :] = skel_row + (1.0 - far_table[0, xx * 8 + j].astype(F32)) * BIG
    row_exp[x] = own_exp[x]

    def row_copies(i):
        leaf, there = x_peers[i - 1], (x + i) % 4
        return [
            remote(row_skel.at[x], row_skel.at[x], row_send.at[0, i - 1], row_recv.at[0, i - 1], leaf),
            remote(own_exp.at[there], row_exp.at[x], row_send.at[1, i - 1], row_recv.at[1, i - 1], leaf),
        ]

    def far_copy(i):
        return remote(
            far_out.at[i - 1], far_in.at[i - 1], row_send.at[2, i - 1], row_recv.at[2, i - 1], x_peers[i - 1]
        )

    for i in range(1, 4):
        for copy in row_copies(i):
            copy.start()
    send_near([1, 2], 1)

    near[...] = jnp.zeros_like(near)

    def near_chunk(slot, c, place):
        inside = (place >= 0) & (place < CLUSTER)
        listed = near_table[0, (place + CLUSTER) % CLUSTER] * inside.astype(jnp.int32)
        row = exponent[...] + (1.0 - listed.astype(F32)) * BIG
        points_c = nb[slot, c, 0:QH, :]

        def weights(h):
            s = dot(points_c, at[h])
            return jnp.exp2(s * LOG2E - row).astype(BF16)

        def value(h):
            start = QH + h * BLOCKS * LANES
            return jnp.concatenate(
                [nb[slot, c, start + b * LANES:start + (b + 1) * LANES, :] for b in range(BLOCKS)], axis=1
            )

        low_w = weights(0)
        high_w = weights(1)
        near[...] += dot(value(0), low_w)
        near[...] += dot(value(1), high_w)

    def some(slot, place, start, stop):
        def visit(c, carry):
            near_chunk(slot, c, place)
            return carry

        lax.fori_loop(start, stop, visit, 0)

    def stage(c):
        near_arrived([3, 4], c)

        def visit(slot, carry):
            other = jnp.where(slot >= PARTNER_DOWN, l + 1 - 2 * k, l)
            place = other + 4 * (slot % 2) - 2
            near_chunk(slot, c, place)
            return carry

        lax.fori_loop(DOWN, PARTNER_UP + 1, visit, 0)

    def forward(c):
        near_arrived([1, 2], c)
        send_near([3, 4, 5], c)

    def add_up(i):
        up_copy(i).wait_recv()
        total = (up_total[k] if i == 0 else up_total[0]) + up_in[i].astype(F32)
        up_total[0] = total
        if i < 4:
            up_out[i + 2] = total.astype(BF16)
            up_copy(i + 1).start()
        return total

    some(OWN, l, 0, 2)
    add_up(0)
    some(OWN, l, 2, 4)
    gather_copy(0).wait_recv()
    gather_copy(1).start()
    near_arrived([0], 0)
    near_arrived([0], 1)
    some(PARTNER, l + 1 - 2 * k, 0, 2)
    add_up(1)
    send_near([1, 2], 2)
    forward(0)
    near_arrived([0], 2)
    near_arrived([0], 3)
    some(PARTNER, l + 1 - 2 * k, 2, 3)
    stage(0)

    add_up(2)
    gather_copy(1).wait_recv()
    gather_copy(2).start()
    send_near([1, 2], 3)
    forward(1)
    some(PARTNER, l + 1 - 2 * k, 3, 4)
    stage(1)

    add_up(3)
    forward(2)
    gather_copy(2).wait_recv()
    for i in range(1, 4):
        for copy in row_copies(i):
            copy.wait_recv()

    def far_visit(i, carry):
        there = (x + i) % 4
        fill_stationary(row_at, row_skel[there])
        rows = row_exp[there]
        items = [(zz, kk) for zz in range(4) for kk in range(2)]
        packs = jnp.concatenate([gathered[kk, zz, 0:LANES, :] for zz, kk in items], axis=0)
        total = jnp.zeros((NRHS, RANK), F32)
        for h in range(2):
            s = dot(packs, row_at[h]) * LOG2E
            weights = jnp.concatenate(
                [jnp.exp2(s[j * LANES:(j + 1) * LANES] - rows[j:j + 1]).astype(BF16) for j in range(8)], axis=0
            )
            value = jnp.concatenate(
                [gathered[kk, zz, (1 + h) * LANES:(2 + h) * LANES, :] for zz, kk in items], axis=1
            )
            total = total + dot(value, weights)
        far_total[i] = total
        return carry

    lax.fori_loop(0, 4, far_visit, 0)
    for i in range(1, 4):
        far_out[i - 1] = far_total[i].astype(BF16)
        far_copy(i).start()
    stage(2)

    upper = add_up(4).astype(BF16)
    cluster_cols = cluster_skel[0].astype(F32)
    fill_stationary(cluster_at, (cluster_cols + cluster_cols).astype(BF16))
    cluster_row, scale = exponent_and_scale(cluster_cols, CLUSTER_SHIFT)
    cluster_exp[...] = cluster_row
    scaled = (upper.astype(F32) * scale).astype(BF16)
    yb[g, 0:LANES, :] = stacked(cluster_cols).T.astype(BF16)
    yb[g, LANES:LANES + half, :] = scaled[:, :LANES]
    yb[g, LANES + half:, :] = scaled[:, LANES:]

    def y_copy(i):
        return remote(yb.at[g], yb.at[g], y_send.at[i], y_recv.at[i], group=y_peers[i])

    for i in range(3):
        y_copy(i).start()
    forward(3)

    def pick(i, carry):
        for j in range(8):
            out[pl.ds(i * 8 + j, 1), :] = target[pl.ds(ordering[0, i * 8 + j], 1), :]
        return carry

    lax.fori_loop(0, LEAF // 8, pick, 0)
    for i in range(3):
        y_copy(i).wait_recv()
    lower = jnp.zeros((half, RANK), F32)
    for h in range(GROUPS):
        row = cluster_exp[...] + (1.0 - cluster_far[0, h].astype(F32)) * BIG
        weights = jnp.concatenate(
            [jnp.exp2(dot(yb[h, 0:LANES, :], cluster_at[i]) * LOG2E - row).astype(BF16) for i in range(2)], axis=0
        )
        value = jnp.concatenate([yb[h, LANES:LANES + half, :], yb[h, LANES + half:, :]], axis=1)
        lower = lower + dot(value, weights)
    low[k] = lower.astype(BF16)
    low_copy = remote(low.at[k], low.at[k], y_send.at[3], y_recv.at[3], partner)
    low_copy.start()
    stage(3)

    for i in range(1, 4):
        far_copy(i).wait_recv()
    low_copy.wait_recv()
    lower_all = jnp.concatenate([low[0], low[1]], axis=0)
    far_sum = (far_total[0] + far_in[0].astype(F32)) + (far_in[1].astype(F32) + far_in[2].astype(F32))
    local_t = far_sum + lax.dot_general(
        lower_all, transfer[0], (((1,), (1,)), ((), ())), preferred_element_type=F32
    )
    local = local_t.astype(BF16).astype(F32).T.astype(BF16)

    def last(c, carry):
        near_copy(5, c).wait_recv()
        near_chunk(FAR_SIDE, c, l + 6 * k - 3)
        return carry

    lax.fori_loop(0, CHUNKS, last, 0)
    for i in range(LEAF // LANES):
        rows = slice(i * LANES, (i + 1) * LANES)
        image = dot(basis[rows, :], local) + near[:, rows].T
        out[rows, :] = iterate[rows, :] + step[...] * (out[rows, :] - image)

    for kind in range(6):
        for c in range(CHUNKS):
            near_copy(kind, c).wait_send()
    for i in range(3):
        gather_copy(i).wait_send()
        y_copy(i).wait_send()
        far_copy(i + 1).wait_send()
        for copy in row_copies(i + 1):
            copy.wait_send()
    for i in range(5):
        up_copy(i).wait_send()
    low_copy.wait_send()


def body(
    points, ordering, iterate, target, step_size, leaf_basis, transfer, leaf_skeleton,
    cluster_skeleton, near_table, far_table, cluster_far,
):
    vmem = pl.BlockSpec(memory_space=pltpu.VMEM)
    smem = pl.BlockSpec(memory_space=pltpu.SMEM)
    dma = pltpu.SemaphoreType.DMA
    return pl.pallas_call(
        kernel,
        out_shape=jax.ShapeDtypeStruct((LEAF, NRHS), F32),
        in_specs=[vmem, smem, vmem, vmem, vmem, vmem, vmem, vmem, vmem, smem, smem, smem],
        out_specs=vmem,
        scratch_shapes=[
            pltpu.VMEM((7, CHUNKS, CHUNK_ROWS, LANES), BF16),
            pltpu.VMEM((2, LANES, LEAF), BF16),
            pltpu.VMEM((1, LEAF), F32),
            pltpu.VMEM((NRHS, LEAF), BF16),
            pltpu.VMEM((NRHS, LEAF), F32),
            pltpu.VMEM((2, 4, 3 * LANES, LANES), BF16),
            pltpu.VMEM((4, DIM, RANK), BF16),
            pltpu.VMEM((4, 8, RANK), F32),
            pltpu.VMEM((4, 8, RANK), F32),
            pltpu.VMEM((2, LANES, RANK), BF16),
            pltpu.VMEM((4, NRHS, RANK), F32),
            pltpu.VMEM((3, NRHS, RANK), BF16),
            pltpu.VMEM((3, NRHS, RANK), BF16),
            pltpu.VMEM((2, NRHS // 2, RANK), F32),
            pltpu.VMEM((6, NRHS // 2, RANK), BF16),
            pltpu.VMEM((5, NRHS // 2, RANK), BF16),
            pltpu.VMEM((GROUPS, LANES + NRHS, LANES), BF16),
            pltpu.VMEM((2, LANES, RANK), BF16),
            pltpu.VMEM((1, RANK), F32),
            pltpu.VMEM((2, NRHS // 2, RANK), BF16),
            dma((6, CHUNKS)), dma((6, CHUNKS)),
            dma((3,)), dma((3,)),
            dma((3, 3)), dma((3, 3)),
            dma((5,)), dma((5,)),
            dma((4,)), dma((4,)),
        ],
        compiler_params=pltpu.CompilerParams(
            collective_id=0, has_side_effects=True, vmem_limit_bytes=56 * 2**20
        ),
    )(
        points.T, ordering, iterate, target, step_size[None, :], leaf_basis, transfer,
        leaf_skeleton.swapaxes(1, 2), cluster_skeleton.swapaxes(1, 2), near_table, far_table, cluster_far,
    )


def solution(mesh):
    both = ("group", "leaf")
    return jax.shard_map(
        body,
        mesh=mesh,
        in_specs=(
            P(both, None), P(both, None), P(both, None), P(both, None), P(), P(both, None),
            P(both, None, None), P(both, None, None), P("group", None, None),
            P(both, None), P(both, None), P("group", None),
        ),
        out_specs=P(both, None),
        check_vma=False,
    )
```

```python
import jax
import jax.numpy as jnp
from jax import lax
from jax.experimental import pallas as pl
from jax.experimental.pallas import tpu as pltpu
from jax.sharding import PartitionSpec as P

LEAF, DIM, NRHS, RANK, CLUSTER, GROUPS = 2048, 64, 128, 256, 32, 4
HALF_LEAF = LEAF // 2
LANES = 128
CHUNKS = 4
QH = HALF_LEAF // CHUNKS
CHUNK_ROWS = 3 * QH
BLOCKS = QH // LANES
LOG2E = 1.4426950408889634
BIG = 1.0e4
POINT_SHIFT, LEAF_SHIFT, CLUSTER_SHIFT = 45.0, 25.0, 45.0
OWN, PARTNER, DOWN, UP, PARTNER_DOWN, PARTNER_UP, FAR_SIDE = range(7)
F32, BF16 = jnp.float32, jnp.bfloat16


def dot(a, b):
    return jnp.dot(a, b, preferred_element_type=F32)


def stacked(cols):
    half = cols.shape[1] // 2
    return jnp.concatenate([cols[:, :half], cols[:, half:]], axis=0)


def exponent_and_scale(cols, shift):
    norm = jnp.sum(cols * cols, axis=0, keepdims=True)
    return (norm + shift) * LOG2E, jnp.exp2((shift - norm) * LOG2E)


def fill_stationary(ref, doubled):
    zeros = jnp.zeros_like(doubled)
    ref[0, 0:DIM, :] = doubled
    ref[0, DIM:, :] = zeros
    ref[1, 0:DIM, :] = zeros
    ref[1, DIM:, :] = doubled


def kernel(
    points, ordering, iterate, target, step, basis, transfer, leaf_skel, cluster_skel,
    near_table, far_table, cluster_far,
    out,
    nb, at, exponent, values, near, gathered, row_skel, row_exp, own_exp, row_at, far_total, far_out, far_in,
    up_total, up_out, up_in, yb, cluster_at, cluster_exp, low,
    near_send, near_recv, gat_send, gat_recv, row_send, row_recv, up_send, up_recv, y_send, y_recv,
):
    g = lax.axis_index("group")
    l = lax.axis_index("leaf")
    x, z, k = l // 8, (l // 2) % 4, l % 2
    half = NRHS // 2

    def at_leaf(xx, zz):
        return (xx % 4) * 8 + (zz % 4) * 2 + k

    partner = x * 8 + z * 2 + (1 - k)
    above, below = (l + 2) % CLUSTER, (l + CLUSTER - 2) % CLUSTER
    side = (l + CLUSTER + 2 * k - 1) % CLUSTER
    z_even, x_even = z % 2, x % 2
    z_first, z_second = at_leaf(x, z + 1 - 2 * z_even), at_leaf(x, z + 3 + 2 * z_even)
    x_first, x_second = at_leaf(x + 1 - 2 * x_even, z), at_leaf(x + 3 + 2 * x_even, z)
    x_peers = [at_leaf(x + i, z) for i in range(1, 4)]
    y_peers = [(g + i) % GROUPS for i in range(1, 4)]

    barrier = pltpu.get_barrier_semaphore()
    for leaf in [partner, above, below, side, z_first, z_second] + x_peers:
        pl.semaphore_signal(barrier, 1, device_id={"leaf": leaf}, device_id_type=pl.DeviceIdType.MESH)
    for group in y_peers:
        pl.semaphore_signal(barrier, 1, device_id={"group": group}, device_id_type=pl.DeviceIdType.MESH)

    def remote(src, dst, send, recv, leaf=None, group=None):
        return pltpu.make_async_remote_copy(
            src_ref=src, dst_ref=dst, send_sem=send, recv_sem=recv,
            device_id={"leaf": leaf} if group is None else {"group": group},
            device_id_type=pl.DeviceIdType.MESH,
        )

    cols = points[...].astype(F32)
    stack = stacked(cols)
    for c in range(CHUNKS):
        nb[OWN, c, 0:QH, :] = stack[:, c * QH:(c + 1) * QH].T.astype(BF16)
    fill_stationary(at, (cols + cols).astype(BF16))
    exponent_row, scale = exponent_and_scale(cols, POINT_SHIFT)
    exponent[...] = exponent_row
    for i in range(LEAF // LANES):
        block = iterate[i * LANES:(i + 1) * LANES, :].astype(BF16).astype(F32).T
        values[:, i * LANES:(i + 1) * LANES] = block.astype(BF16)
        high, j = divmod(i, HALF_LEAF // LANES)
        c, b = divmod(j, BLOCKS)
        start = QH + LANES * (high * BLOCKS + b)
        nb[OWN, c, start:start + LANES, :] = (
            block * scale[:, i * LANES:(i + 1) * LANES]
        ).astype(BF16)

    pl.semaphore_wait(barrier, 12)

    def near_copy(kind, c):
        src, dst, leaf = [
            (OWN, PARTNER, partner),
            (OWN, DOWN, above),
            (OWN, UP, below),
            (DOWN, PARTNER_DOWN, partner),
            (UP, PARTNER_UP, partner),
            (DOWN + 1 - k, FAR_SIDE, side),
        ][kind]
        return remote(nb.at[src, c], nb.at[dst, c], near_send.at[kind, c], near_recv.at[dst - 1, c], leaf)

    def send_near(kinds, c):
        for kind in kinds:
            near_copy(kind, c).start()

    def near_arrived(kinds, c):
        for kind in kinds:
            near_copy(kind, c).wait_recv()

    send_near([1, 2], 0)
    for c in range(CHUNKS):
        send_near([0], c)

    coef = dot(values[...], basis[...]).astype(BF16)
    skel = leaf_skel[0].astype(F32)
    skel_row, scale = exponent_and_scale(skel, LEAF_SHIFT)
    scaled = (coef.astype(F32) * scale).astype(BF16)
    gathered[k, z, 0:LANES, :] = stacked(skel).T.astype(BF16)
    gathered[k, z, LANES:2 * LANES, :] = scaled[:, :LANES]
    gathered[k, z, 2 * LANES:, :] = scaled[:, LANES:]

    def gather_copy(i):
        part = [gathered.at[k, z], gathered.at[k, pl.ds(2 * (z // 2), 2)], gathered.at[k]][i]
        return remote(part, part, gat_send.at[i], gat_recv.at[i], [z_first, z_second, partner][i])

    gather_copy(0).start()
    lifted = dot(coef, transfer[0])
    for i in range(2):
        up_total[i] = lifted[i * half:(i + 1) * half]
        up_out[i] = lifted[i * half:(i + 1) * half].astype(BF16)

    def up_copy(i):
        src = up_out.at[1 - k] if i == 0 else up_out.at[i + 1]
        leaf = [partner, z_first, z_second, x_first, x_second][i]
        return remote(src, up_in.at[i], up_send.at[i], up_recv.at[i], leaf)

    up_copy(0).start()

    row_skel[x] = (skel + skel).astype(BF16)
    for xx in range(4):
        for j in range(8):
            own_exp[xx, j:j + 1, :] = skel_row + (1.0 - far_table[0, xx * 8 + j].astype(F32)) * BIG
    row_exp[x] = own_exp[x]

    def row_copies(i):
        leaf, there = x_peers[i - 1], (x + i) % 4
        return [
            remote(row_skel.at[x], row_skel.at[x], row_send.at[0, i - 1], row_recv.at[0, i - 1], leaf),
            remote(own_exp.at[there], row_exp.at[x], row_send.at[1, i - 1], row_recv.at[1, i - 1], leaf),
        ]

    def far_copy(i):
        return remote(
            far_out.at[i - 1], far_in.at[i - 1], row_send.at[2, i - 1], row_recv.at[2, i - 1], x_peers[i - 1]
        )

    for i in range(1, 4):
        for copy in row_copies(i):
            copy.start()

    near[...] = jnp.zeros_like(near)

    def near_chunk(slot, c, place):
        inside = (place >= 0) & (place < CLUSTER)
        listed = near_table[0, (place + CLUSTER) % CLUSTER] * inside.astype(jnp.int32)
        row = exponent[...] + (1.0 - listed.astype(F32)) * BIG
        points_c = nb[slot, c, 0:QH, :]

        def weights(h):
            s = dot(points_c, at[h])
            return jnp.exp2(s * LOG2E - row).astype(BF16)

        def value(h):
            start = QH + h * BLOCKS * LANES
            return jnp.concatenate(
                [nb[slot, c, start + b * LANES:start + (b + 1) * LANES, :] for b in range(BLOCKS)], axis=1
            )

        low_w = weights(0)
        high_w = weights(1)
        near[...] += dot(value(0), low_w)
        near[...] += dot(value(1), high_w)

    def some(slot, place, start, stop):
        def visit(c, carry):
            near_chunk(slot, c, place)
            return carry

        lax.fori_loop(start, stop, visit, 0)

    def stage(c):
        def visit(slot, carry):
            center = jnp.where(slot >= PARTNER_DOWN, l + 1 - 2 * k, l)
            near_chunk(slot, c, center + 4 * (slot % 2) - 2)
            return carry

        near_arrived([1, 2], c)
        send_near([3, 4, 5], c)
        lax.fori_loop(DOWN, PARTNER_DOWN, visit, 0)
        near_arrived([3, 4], c)
        lax.fori_loop(PARTNER_DOWN, FAR_SIDE, visit, 0)

    def add_up(i):
        up_copy(i).wait_recv()
        total = (up_total[k] if i == 0 else up_total[0]) + up_in[i].astype(F32)
        up_total[0] = total
        if i < 4:
            up_out[i + 2] = total.astype(BF16)
            up_copy(i + 1).start()
        return total

    other = l + 1 - 2 * k
    some(OWN, l, 0, 4)
    add_up(0)
    send_near([1, 2], 1)
    near_arrived([0], 0)
    near_arrived([0], 1)
    some(PARTNER, other, 0, 2)
    gather_copy(0).wait_recv()
    gather_copy(1).start()
    near_arrived([0], 2)
    near_arrived([0], 3)
    some(PARTNER, other, 2, 4)
    add_up(1)
    send_near([1, 2], 2)

    def pick(i, carry):
        for j in range(8):
            out[pl.ds(i * 8 + j, 1), :] = target[pl.ds(ordering[0, i * 8 + j], 1), :]
        return carry

    lax.fori_loop(0, LEAF // 8, pick, 0)
    add_up(2)
    gather_copy(1).wait_recv()
    gather_copy(2).start()
    send_near([1, 2], 3)
    stage(0)
    add_up(3)
    gather_copy(2).wait_recv()
    for i in range(1, 4):
        for copy in row_copies(i):
            copy.wait_recv()

    def far_visit(i, carry):
        there = (x + i) % 4
        fill_stationary(row_at, row_skel[there])
        rows = row_exp[there]
        items = [(zz, kk) for zz in range(4) for kk in range(2)]
        packs = jnp.concatenate([gathered[kk, zz, 0:LANES, :] for zz, kk in items], axis=0)
        total = jnp.zeros((NRHS, RANK), F32)
        for h in range(2):
            s = dot(packs, row_at[h]) * LOG2E
            weights = jnp.concatenate(
                [jnp.exp2(s[j * LANES:(j + 1) * LANES] - rows[j:j + 1]).astype(BF16) for j in range(8)], axis=0
            )
            value = jnp.concatenate(
                [gathered[kk, zz, (1 + h) * LANES:(2 + h) * LANES, :] for zz, kk in items], axis=1
            )
            total = total + dot(value, weights)
        far_total[i] = total
        return carry

    lax.fori_loop(0, 4, far_visit, 0)
    for i in range(1, 4):
        far_out[i - 1] = far_total[i].astype(BF16)
        far_copy(i).start()
    stage(1)
    upper = add_up(4).astype(BF16)
    cluster_cols = cluster_skel[0].astype(F32)
    fill_stationary(cluster_at, (cluster_cols + cluster_cols).astype(BF16))
    cluster_row, scale = exponent_and_scale(cluster_cols, CLUSTER_SHIFT)
    cluster_exp[...] = cluster_row
    scaled = (upper.astype(F32) * scale).astype(BF16)
    yb[g, 0:LANES, :] = stacked(cluster_cols).T.astype(BF16)
    yb[g, LANES:LANES + half, :] = scaled[:, :LANES]
    yb[g, LANES + half:, :] = scaled[:, LANES:]

    def y_copy(i):
        return remote(yb.at[g], yb.at[g], y_send.at[i], y_recv.at[i], group=y_peers[i])

    for i in range(3):
        y_copy(i).start()
    stage(2)
    for i in range(3):
        y_copy(i).wait_recv()
    lower = jnp.zeros((half, RANK), F32)
    for h in range(GROUPS):
        row = cluster_exp[...] + (1.0 - cluster_far[0, h].astype(F32)) * BIG
        weights = jnp.concatenate(
            [jnp.exp2(dot(yb[h, 0:LANES, :], cluster_at[i]) * LOG2E - row).astype(BF16) for i in range(2)], axis=0
        )
        value = jnp.concatenate([yb[h, LANES:LANES + half, :], yb[h, LANES + half:, :]], axis=1)
        lower = lower + dot(value, weights)
    low[k] = lower.astype(BF16)
    low_copy = remote(low.at[k], low.at[k], y_send.at[3], y_recv.at[3], partner)
    low_copy.start()
    stage(3)

    def last(c, carry):
        near_copy(5, c).wait_recv()
        near_chunk(FAR_SIDE, c, l + 6 * k - 3)
        return carry

    lax.fori_loop(0, CHUNKS, last, 0)
    for i in range(1, 4):
        far_copy(i).wait_recv()
    low_copy.wait_recv()
    lower_all = jnp.concatenate([low[0], low[1]], axis=0)
    far_sum = (far_total[0] + far_in[0].astype(F32)) + (far_in[1].astype(F32) + far_in[2].astype(F32))
    local_t = far_sum + lax.dot_general(
        lower_all, transfer[0], (((1,), (1,)), ((), ())), preferred_element_type=F32
    )
    local = local_t.astype(BF16).astype(F32).T.astype(BF16)

    for i in range(LEAF // LANES):
        rows = slice(i * LANES, (i + 1) * LANES)
        image = dot(basis[rows, :], local) + near[:, rows].T
        out[rows, :] = iterate[rows, :] + step[...] * (out[rows, :] - image)

    for kind in range(6):
        for c in range(CHUNKS):
            near_copy(kind, c).wait_send()
    for i in range(3):
        gather_copy(i).wait_send()
        y_copy(i).wait_send()
        far_copy(i + 1).wait_send()
        for copy in row_copies(i + 1):
            copy.wait_send()
    for i in range(5):
        up_copy(i).wait_send()
    low_copy.wait_send()


def body(
    points, ordering, iterate, target, step_size, leaf_basis, transfer, leaf_skeleton,
    cluster_skeleton, near_table, far_table, cluster_far,
):
    vmem = pl.BlockSpec(memory_space=pltpu.VMEM)
    smem = pl.BlockSpec(memory_space=pltpu.SMEM)
    dma = pltpu.SemaphoreType.DMA
    return pl.pallas_call(
        kernel,
        out_shape=jax.ShapeDtypeStruct((LEAF, NRHS), F32),
        in_specs=[vmem, smem, vmem, vmem, vmem, vmem, vmem, vmem, vmem, smem, smem, smem],
        out_specs=vmem,
        scratch_shapes=[
            pltpu.VMEM((7, CHUNKS, CHUNK_ROWS, LANES), BF16),
            pltpu.VMEM((2, LANES, LEAF), BF16),
            pltpu.VMEM((1, LEAF), F32),
            pltpu.VMEM((NRHS, LEAF), BF16),
            pltpu.VMEM((NRHS, LEAF), F32),
            pltpu.VMEM((2, 4, 3 * LANES, LANES), BF16),
            pltpu.VMEM((4, DIM, RANK), BF16),
            pltpu.VMEM((4, 8, RANK), F32),
            pltpu.VMEM((4, 8, RANK), F32),
            pltpu.VMEM((2, LANES, RANK), BF16),
            pltpu.VMEM((4, NRHS, RANK), F32),
            pltpu.VMEM((3, NRHS, RANK), BF16),
            pltpu.VMEM((3, NRHS, RANK), BF16),
            pltpu.VMEM((2, NRHS // 2, RANK), F32),
            pltpu.VMEM((6, NRHS // 2, RANK), BF16),
            pltpu.VMEM((5, NRHS // 2, RANK), BF16),
            pltpu.VMEM((GROUPS, LANES + NRHS, LANES), BF16),
            pltpu.VMEM((2, LANES, RANK), BF16),
            pltpu.VMEM((1, RANK), F32),
            pltpu.VMEM((2, NRHS // 2, RANK), BF16),
            dma((6, CHUNKS)), dma((6, CHUNKS)),
            dma((3,)), dma((3,)),
            dma((3, 3)), dma((3, 3)),
            dma((5,)), dma((5,)),
            dma((4,)), dma((4,)),
        ],
        compiler_params=pltpu.CompilerParams(
            collective_id=0, has_side_effects=True, vmem_limit_bytes=56 * 2**20
        ),
    )(
        points.T, ordering, iterate, target, step_size[None, :], leaf_basis, transfer,
        leaf_skeleton.swapaxes(1, 2), cluster_skeleton.swapaxes(1, 2), near_table, far_table, cluster_far,
    )


def solution(mesh):
    both = ("group", "leaf")
    return jax.shard_map(
        body,
        mesh=mesh,
        in_specs=(
            P(both, None), P(both, None), P(both, None), P(both, None), P(), P(both, None),
            P(both, None, None), P(both, None, None), P("group", None, None),
            P(both, None), P(both, None), P("group", None),
        ),
        out_specs=P(both, None),
        check_vma=False,
    )
```
